32 devices in a mesh: slab: 8 (over z, x), tile: 4 (over y, core).
Axes of the slice: x: 2, y: 2, z: 4, core: 2. Of those that a mesh axis runs over, the one named last changes fastest.
Arguments:
- tiles: bfloat16 [32, 20, 256, 128], P(('slab', 'tile')), may hold values from -6 to 6
- offsets: int32 [32, 2], replicated, may hold values from -3 to 690, as said below
- fracs: int32 [32, 3], replicated, may hold values from 0 to 15
Outputs:
- joined: bfloat16 [128, 946, 128], P(('slab', 'tile'))
The draws below stay inside these ranges and needn't reach their ends.
Inputs may be any that keep to these rules, and one draw needn't show every extreme that they name: offsets[g, 0] lies within 1 of (g // 4) * 16 - 2, and offsets[g, 1] within 4 of (g % 4) * 230, clipped to 0 .. 690; some tile reaches each end of the plane shift.
All inputs are finite; a program needn't handle non-finite values.
Results may differ from the reference program's by a relative error of at most 0.0038.
Values may be sent and summed in bfloat16 or wider, within the bound.
A program may use at most 64 MiB of HBM per device.

```python
import jax
import jax.numpy as jnp
from jax import lax

GROUPZ = 16
MARGIN = 2
JIT = 1
TY = 256
TX = 128
STEPY = 230
JITY = 4
RY = 26
RX = 16
QUANT = 16
TZ = 20
TILES_GROUP = 4
TILES = 32
MY = 946
NZ = 128


def draw_offsets(key, part):
    key_plane = jax.random.fold_in(key, 11)
    key_row = jax.random.fold_in(key, 12)
    key_lowest = jax.random.fold_in(key, 13)
    key_highest = jax.random.fold_in(key, 14)
    position = jnp.arange(TILES, dtype=jnp.int32)
    group_of = position // TILES_GROUP
    within = position % TILES_GROUP
    shift_plane = jax.random.randint(key_plane, (TILES,), -JIT, JIT + 1)
    lowest_tile = jax.random.randint(key_lowest, (), 0, TILES)
    highest_tile = (lowest_tile + 1 + jax.random.randint(key_highest, (), 0, TILES - 1)) % TILES
    shift_plane = jnp.where(position == lowest_tile, -JIT, shift_plane)
    shift_plane = jnp.where(position == highest_tile, JIT, shift_plane)
    first_plane = group_of * GROUPZ - MARGIN + shift_plane
    shift_row = jax.random.randint(key_row, (TILES,), -JITY, JITY + 1)
    first_row = jnp.clip(within * STEPY + shift_row, 0, MY - TY)
    return jnp.stack([first_plane, first_row], axis=1).astype(jnp.int32)


def set_ends(drawn, key, low, largest):
    shape = drawn.shape
    index_at = [jax.random.randint(jax.random.fold_in(key, axis), (), 0, shape[axis]) for axis in range(len(shape))]
    drawn = drawn.at[tuple(index_at)].set(low)
    longest = shape.index(max(shape))
    index_at[longest] = (index_at[longest] + 1) % shape[longest]
    return drawn.at[tuple(index_at)].set(largest)


def levels(key, shape, pieces, least, top_value):
    def one(dim, shards_of):
        draws = jax.random.uniform(jax.random.fold_in(jax.random.fold_in(key, 6), dim), (shards_of,), jnp.float32, least / len(pieces), top_value / len(pieces))
        return jnp.repeat(jnp.exp(draws), shape[dim] // shards_of).reshape((-1,) + (1,) * (len(shape) - dim - 1))

    level = one(*pieces[0])
    for cut in pieces[1:]:
        level = level * one(*cut)
    return level


def centred(own_key, shape, scale, most, shards=(), held_as=jnp.bfloat16):
    entries = scale * jax.random.normal(own_key, shape, jnp.float32)
    if shards:
        entries = entries * levels(own_key, shape, shards, -0.22, 0.18)
    return jnp.clip(entries, -most, most).astype(held_as)


def setup_inputs(seed: int = 0) -> dict:
    splits = jax.random.split(jax.random.key(seed), 4)
    tiles = centred(splits[0], (TILES, TZ, TY, TX), 1.0, 6.0, ((0, 32),))
    offsets = draw_offsets(jax.random.fold_in(splits[3], 71), 0)
    fracs = set_ends(jax.random.randint(splits[2], (TILES, 3), 0, QUANT), jax.random.fold_in(splits[2], 1), 0, QUANT - 1).astype(jnp.int32)
    return {"tiles": tiles, "offsets": offsets, "fracs": fracs}


weight_floor = 0.05


def ramp(length, ramp_width):
    position = jnp.arange(length, dtype=jnp.float32)
    rising = 0.5 - 0.5 * jnp.cos(jnp.pi * (position + 1.0) / (ramp_width + 1.0))
    rising = jnp.where(position < ramp_width, rising, jnp.ones_like(rising))
    return jnp.minimum(rising, rising[::-1])


def resample(raw_tile, fraction_row):
    volume_field = raw_tile.astype(jnp.float32)
    for direction in range(3):
        fraction = fraction_row[direction].astype(jnp.float32) / QUANT
        extent = volume_field.shape[direction]
        shifted = jnp.concatenate([lax.slice_in_dim(volume_field, 1, extent, axis=direction), jnp.zeros_like(lax.slice_in_dim(volume_field, 0, 1, axis=direction))], axis=direction)
        volume_field = (1.0 - fraction) * volume_field + fraction * shifted
    return volume_field


def reference(tiles, offsets, fracs):
    ramp_z = ramp(TZ, 2 * MARGIN)
    ramp_y = ramp(TY, RY)
    ramp_x = ramp(TX, RX)
    weight = ramp_z[:, None, None] * ramp_y[None, :, None] * ramp_x[None, None, :]
    border = MARGIN + JIT
    numer_init = jnp.zeros((NZ + 2 * border, MY, TX), jnp.float32)
    weight_init = jnp.zeros((NZ + 2 * border, MY, TX), jnp.float32)

    def place(totals, element):
        numer, weight_sum = totals
        one_tile, corner, fraction_row = element
        blended = (resample(one_tile, fraction_row) * weight).astype(jnp.bfloat16)
        start_at = ((corner[0] + border).astype(jnp.int32), corner[1].astype(jnp.int32), jnp.zeros((), jnp.int32))
        current = lax.dynamic_slice(numer, start_at, (TZ, TY, TX))
        numer = lax.dynamic_update_slice(numer, current + blended.astype(jnp.float32), start_at)
        current = lax.dynamic_slice(weight_sum, start_at, (TZ, TY, TX))
        weight_sum = lax.dynamic_update_slice(weight_sum, current + weight, start_at)
        return (numer, weight_sum), None

    (numer, weight_sum), _ = lax.scan(place, (numer_init, weight_init), (tiles, offsets, fracs))
    numer = numer[border:border + NZ]
    weight_sum = weight_sum[border:border + NZ]
    return (numer / jnp.maximum(weight_sum, weight_floor)).astype(jnp.bfloat16)
```

```python
import functools

import jax
import jax.numpy as jnp
import numpy as np
from jax import lax
from jax.experimental import pallas as pl
from jax.experimental.pallas import tpu as pltpu
from jax.sharding import PartitionSpec as P

GROUPZ = 16
MARGIN = 2
JIT = 1
STEPY = 230
JITY = 4
RY = 26
RX = 16
QUANT = 16
EDGE = MARGIN + JIT
PADY = 16
PADZ = 24

weight_floor = 0.05
MESH = pl.DeviceIdType.MESH


def ramp(length, ramp_width):
    position = np.arange(length, dtype=np.float64)
    rising = 0.5 - 0.5 * np.cos(np.pi * (position + 1.0) / (ramp_width + 1.0))
    rising = np.where(position < ramp_width, rising, 1.0)
    return np.minimum(rising, rising[::-1])


def frame_start(rank):
    if isinstance(rank, int):
        return max((rank * STEPY - JITY) // 8 * 8, 0)
    return jnp.maximum((rank * STEPY + 8 - JITY) // 8 * 8 - 8, 0)


def round_up(value, step):
    return -(-value // step) * step


def kernel(
    groups, n, per, depth, tile_rows, frame, acc_rows,
    offs, fracs, rampz, table, tile_ref, out_ref,
    raw, coef, wa, wb, blend, edge_send, edge_recv, recv, acc, rec,
    load_sem, es_sem, er_sem, s_sem, r_sem,
):
    g = lax.axis_index("slab")
    r = lax.axis_index("tile")
    me = g * n + r
    low = r < n // 2
    cols = raw.shape[2]
    last = n - 1

    load = pltpu.make_async_copy(tile_ref.at[0], raw.at[pl.ds(0, depth)], load_sem)
    load.start()

    barrier = pltpu.get_barrier_semaphore()
    for i in range(1, n):
        pl.semaphore_signal(
            barrier, inc=1, device_id=(g, lax.rem(r + i, n)), device_id_type=MESH
        )
    has_below = g > 0
    has_above = g < groups - 1

    @pl.when(has_below)
    def _():
        pl.semaphore_signal(barrier, inc=1, device_id=(g - 1, r), device_id_type=MESH)

    @pl.when(has_above)
    def _():
        pl.semaphore_signal(barrier, inc=1, device_id=(g + 1, r), device_id_type=MESH)

    def table_row(at):
        return jnp.clip(at, 0, table.shape[0] - frame)

    def rampz_at(z):
        return rampz[jnp.clip(z + PADZ, 0, rampz.shape[0] - 1)]

    corner = offs[0, me]
    shift = offs[1, me] - frame_start(r)
    fz = fracs[0, me].astype(jnp.float32) / QUANT
    fy = fracs[1, me].astype(jnp.float32) / QUANT
    fx = fracs[2, me].astype(jnp.float32) / QUANT
    row = lax.broadcasted_iota(jnp.int32, (frame, tile_rows), 0)
    col = lax.broadcasted_iota(jnp.int32, (frame, tile_rows), 1)
    behind = col - row + shift
    lerp_y = jnp.where(behind == 0, 1.0 - fy, jnp.where(behind == 1, fy, 0.0))
    coef[:, :tile_rows] = ((1.0 - fz) * lerp_y).astype(jnp.bfloat16)
    coef[:, tile_rows:] = (fz * lerp_y).astype(jnp.bfloat16)
    weight = table[pl.ds(table_row(PADY - shift), frame), :]
    lane = lax.broadcasted_iota(jnp.int32, (frame, cols), 1)
    wa[...] = weight * (1.0 - fx)
    wb[...] = jnp.where(lane < cols - 1, weight * fx, 0.0)
    raw[depth] = jnp.zeros(raw.shape[1:], raw.dtype)

    def planes(store, first, count):
        at = [jnp.clip(first + j, 0, depth - 1) for j in range(count)]
        top = jnp.concatenate([raw[z] for z in at], axis=1)
        bottom = jnp.concatenate([raw[z + 1] for z in at], axis=1)
        mixed = jnp.dot(
            coef[...], jnp.concatenate([top, bottom], axis=0),
            preferred_element_type=jnp.float32,
        )
        for j in range(count):
            part = mixed[:, j * cols : (j + 1) * cols]
            value = part * wa[...] + pltpu.roll(part, cols - 1, 1) * wb[...]
            store(j, (value * rampz_at(first + j)).astype(jnp.bfloat16))

    base = g * GROUPZ - corner

    def mirrored(owner):
        return jnp.where(low, owner, last - owner)

    def blend_owner(owner):
        def store(j, value):
            blend[owner, j] = value

        planes(store, base + owner * per, per)

    def send_owner(owner):
        @pl.when(owner != r)
        def _():
            pltpu.make_async_remote_copy(
                src_ref=blend.at[owner], dst_ref=recv.at[r],
                send_sem=s_sem.at[owner], recv_sem=r_sem.at[r],
                device_id=(g, owner), device_id_type=MESH,
            ).start()

    def edge_copy(side):
        return pltpu.make_async_remote_copy(
            src_ref=edge_send.at[side], dst_ref=edge_recv.at[side],
            send_sem=es_sem.at[side], recv_sem=er_sem.at[side],
            device_id=(g + 1 - 2 * side, r), device_id_type=MESH,
        )

    def sends_to(side):
        return jnp.where(side == 0, g < groups - 1, g > 0)

    def gets_from(side):
        return jnp.where(side == 0, g > 0, g < groups - 1)

    def send_edge(side):
        def store(j, value):
            edge_send[side, j] = value

        planes(store, base + jnp.where(side == 0, GROUPZ, -EDGE), EDGE)

        @pl.when(sends_to(side))
        def _():
            edge_copy(side).start()

    edge_planes = list(range(EDGE)) + list(range(GROUPZ - EDGE, GROUPZ))
    bound = sorted({q // per for q in edge_planes}, reverse=True)
    free = [o for o in range(last, -1, -1) if o not in bound]
    far_side = jnp.where(low, 1, 0)

    load.wait()
    pl.semaphore_wait(barrier, n - 1 + jnp.where(has_below, 1, 0) + jnp.where(has_above, 1, 0))
    send_edge(far_side)
    for o in free[: len(free) // 2]:
        blend_owner(mirrored(o))
        send_owner(mirrored(o))
    send_edge(1 - far_side)
    for o in free[len(free) // 2 :]:
        blend_owner(mirrored(o))
        send_owner(mirrored(o))
    for o in bound:
        blend_owner(mirrored(o))

    for step in range(2):
        side = far_side if step == 0 else 1 - far_side

        @pl.when(gets_from(side))
        def _():
            edge_copy(side).wait_recv()
            for p in range(EDGE):
                q = p + jnp.where(side == 0, 0, GROUPZ - EDGE)
                owner, j = q // per, q % per
                blend[owner, j] = (
                    blend[owner, j].astype(jnp.float32)
                    + edge_recv[side, p].astype(jnp.float32)
                ).astype(jnp.bfloat16)

        for o in bound:
            if (o >= n // 2) == (step == 0):
                send_owner(mirrored(o))

    rec[...] = jnp.zeros_like(rec)
    for k in range(n):
        s = frame_start(k)
        totals = [0.0] * per
        for delta in (-1, 0, 1):
            group = jnp.clip(g + delta, 0, groups - 1)
            exists = jnp.where(group == g + delta, 1.0, 0.0)
            z0 = offs[0, group * n + k]
            wy = table[pl.ds(table_row(PADY + s - offs[1, group * n + k]), frame), :]
            for j in range(per):
                z = g * GROUPZ + r * per + j - z0
                totals[j] = totals[j] + wy * (rampz_at(z) * exists)
        for j in range(per):
            rec[j, s : s + frame] = rec[j, s : s + frame] + totals[j]
    rec[...] = 1.0 / jnp.maximum(rec[...], weight_floor)

    acc[...] = jnp.zeros_like(acc)

    def add(k, source):
        s = pl.multiple_of(frame_start(k), 8)
        for j in range(per):
            acc[j, pl.ds(s, frame)] = acc[j, pl.ds(s, frame)] + source[j].astype(jnp.float32)

    add(r, blend.at[r])
    for i in range(1, n):
        k = ((r // 2 + i // 2) % (n // 2)) * 2 + (r + i) % 2
        pltpu.make_async_remote_copy(
            src_ref=blend.at[r], dst_ref=recv.at[k],
            send_sem=s_sem.at[k], recv_sem=r_sem.at[k],
            device_id=(g, k), device_id_type=MESH,
        ).wait_recv()
        add(k, recv.at[k])
    rows = out_ref.shape[1]
    for j in range(per):
        out_ref[j] = (acc[j, :rows] * rec[j, :rows]).astype(jnp.bfloat16)

    for i in range(1, n):
        k = lax.rem(r + i, n)
        pltpu.make_async_remote_copy(
            src_ref=blend.at[k], dst_ref=recv.at[r],
            send_sem=s_sem.at[k], recv_sem=r_sem.at[r],
            device_id=(g, k), device_id_type=MESH,
        ).wait_send()
    for side in range(2):
        @pl.when(sends_to(side))
        def _():
            edge_copy(side).wait_send()


def solution(mesh):
    groups, n = mesh.shape["slab"], mesh.shape["tile"]

    def shards(tiles, offsets, fracs):
        _, depth, tile_rows, cols = tiles.shape
        per = GROUPZ // n
        rows = (n - 1) * STEPY + tile_rows
        reach = max(
            min(k * STEPY + JITY, rows - tile_rows) + tile_rows - frame_start(k) for k in range(n)
        )
        frame = round_up(reach, 16)
        acc_rows = round_up(max(rows, frame_start(n - 1) + frame), 16)
        plane = ramp(tile_rows, RY)[:, None] * ramp(cols, RX)[None, :]
        table = np.zeros((round_up(PADY + frame + 8, 8), cols), np.float32)
        table[PADY : PADY + tile_rows] = plane
        rampz = np.zeros((depth + 2 * PADZ,), np.float32)
        rampz[PADZ : PADZ + depth] = ramp(depth, 2 * MARGIN)
        bf16, f32 = jnp.bfloat16, jnp.float32
        dma = pltpu.SemaphoreType.DMA
        return pl.pallas_call(
            functools.partial(kernel, groups, n, per, depth, tile_rows, frame, acc_rows),
            out_shape=jax.ShapeDtypeStruct((per, rows, cols), bf16),
            in_specs=[pl.BlockSpec(memory_space=pltpu.SMEM)] * 3
            + [pl.BlockSpec(memory_space=pltpu.VMEM), pl.BlockSpec(memory_space=pl.ANY)],
            out_specs=pl.BlockSpec(memory_space=pltpu.VMEM),
            scratch_shapes=[
                pltpu.VMEM((depth + 1, tile_rows, cols), bf16),
                pltpu.VMEM((frame, 2 * tile_rows), bf16),
                pltpu.VMEM((frame, cols), f32),
                pltpu.VMEM((frame, cols), f32),
                pltpu.VMEM((n, per, frame, cols), bf16),
                pltpu.VMEM((2, EDGE, frame, cols), bf16),
                pltpu.VMEM((2, EDGE, frame, cols), bf16),
                pltpu.VMEM((n, per, frame, cols), bf16),
                pltpu.VMEM((per, acc_rows, cols), f32),
                pltpu.VMEM((per, acc_rows, cols), f32),
                dma, dma((2,)), dma((2,)), dma((n,)), dma((n,)),
            ],
            compiler_params=pltpu.CompilerParams(collective_id=0, has_side_effects=True),
        )(offsets.T, fracs.T, jnp.asarray(rampz), jnp.asarray(table), tiles)

    in_specs = (P(("slab", "tile"), None, None, None), P(), P())
    out_specs = P(("slab", "tile"), None, None)
    return jax.shard_map(shards, mesh=mesh, in_specs=in_specs, out_specs=out_specs, check_vma=False)
```

```python
import functools

import jax
import jax.numpy as jnp
import numpy as np
from jax import lax
from jax.experimental import pallas as pl
from jax.experimental.pallas import tpu as pltpu
from jax.sharding import PartitionSpec as P

GROUPZ = 16
MARGIN = 2
JIT = 1
STEPY = 230
JITY = 4
RY = 26
RX = 16
QUANT = 16
EDGE = MARGIN + JIT
PADY = 16
PADZ = 24

weight_floor = 0.05
MESH = pl.DeviceIdType.MESH


def ramp(length, ramp_width):
    position = np.arange(length, dtype=np.float64)
    rising = 0.5 - 0.5 * np.cos(np.pi * (position + 1.0) / (ramp_width + 1.0))
    rising = np.where(position < ramp_width, rising, 1.0)
    return np.minimum(rising, rising[::-1])


def frame_start(rank):
    if isinstance(rank, int):
        return max((rank * STEPY - JITY) // 8 * 8, 0)
    return jnp.maximum((rank * STEPY + 8 - JITY) // 8 * 8 - 8, 0)


def round_up(value, step):
    return -(-value // step) * step


def kernel(
    groups, n, per, depth, tile_rows, frame, acc_rows,
    offs, fracs, rampz, table, tile_ref, out_ref,
    raw, coef, wa, wb, blend, edge_send, edge_recv, recv, acc, rec,
    load_sem, es_sem, er_sem, s_sem, r_sem,
):
    g = lax.axis_index("slab")
    r = lax.axis_index("tile")
    me = g * n + r
    low = r < n // 2
    cols = raw.shape[2]
    last = n - 1

    load = pltpu.make_async_copy(tile_ref.at[0], raw.at[pl.ds(0, depth)], load_sem)
    load.start()

    barrier = pltpu.get_barrier_semaphore()
    for i in range(1, n):
        pl.semaphore_signal(
            barrier, inc=1, device_id=(g, lax.rem(r + i, n)), device_id_type=MESH
        )
    has_below = g > 0
    has_above = g < groups - 1

    @pl.when(has_below)
    def _():
        pl.semaphore_signal(barrier, inc=1, device_id=(g - 1, r), device_id_type=MESH)

    @pl.when(has_above)
    def _():
        pl.semaphore_signal(barrier, inc=1, device_id=(g + 1, r), device_id_type=MESH)

    def table_row(at):
        return jnp.clip(at, 0, table.shape[0] - frame)

    def rampz_at(z):
        return rampz[jnp.clip(z + PADZ, 0, rampz.shape[0] - 1)]

    corner = offs[0, me]
    shift = offs[1, me] - frame_start(r)
    fz = fracs[0, me].astype(jnp.float32) / QUANT
    fy = fracs[1, me].astype(jnp.float32) / QUANT
    fx = fracs[2, me].astype(jnp.float32) / QUANT
    row = lax.broadcasted_iota(jnp.int32, (frame, tile_rows), 0)
    col = lax.broadcasted_iota(jnp.int32, (frame, tile_rows), 1)
    behind = col - row + shift
    lerp_y = jnp.where(behind == 0, 1.0 - fy, jnp.where(behind == 1, fy, 0.0))
    coef[:, :tile_rows] = ((1.0 - fz) * lerp_y).astype(jnp.bfloat16)
    coef[:, tile_rows:] = (fz * lerp_y).astype(jnp.bfloat16)
    weight = table[pl.ds(table_row(PADY - shift), frame), :]
    lane = lax.broadcasted_iota(jnp.int32, (frame, cols), 1)
    wa[...] = weight * (1.0 - fx)
    wb[...] = jnp.where(lane < cols - 1, weight * fx, 0.0)
    raw[depth] = jnp.zeros(raw.shape[1:], raw.dtype)

    def planes(store, first, count):
        at = [jnp.clip(first + j, 0, depth - 1) for j in range(count)]
        top = jnp.concatenate([raw[z] for z in at], axis=1)
        bottom = jnp.concatenate([raw[z + 1] for z in at], axis=1)
        mixed = jnp.dot(
            coef[...], jnp.concatenate([top, bottom], axis=0),
            preferred_element_type=jnp.float32,
        )
        for j in range(count):
            part = mixed[:, j * cols : (j + 1) * cols]
            value = part * wa[...] + pltpu.roll(part, cols - 1, 1) * wb[...]
            store(j, (value * rampz_at(first + j)).astype(jnp.bfloat16))

    base = g * GROUPZ - corner

    def mirrored(owner):
        return jnp.where(low, owner, last - owner)

    def blend_owner(owner):
        def store(j, value):
            blend[owner, j] = value

        planes(store, base + owner * per, per)

    def send_owner(owner):
        @pl.when(owner != r)
        def _():
            pltpu.make_async_remote_copy(
                src_ref=blend.at[owner], dst_ref=recv.at[r],
                send_sem=s_sem.at[owner], recv_sem=r_sem.at[r],
                device_id=(g, owner), device_id_type=MESH,
            ).start()

    def send_part(owner, first, count):
        if count:
            @pl.when(owner != r)
            def _():
                part = pl.ds(first, count)
                pltpu.make_async_remote_copy(
                    src_ref=blend.at[owner, part], dst_ref=recv.at[r, part],
                    send_sem=s_sem.at[owner], recv_sem=r_sem.at[r],
                    device_id=(g, owner), device_id_type=MESH,
                ).start()

    def edge_count(o):
        o = max(o, last - o)
        return sum(1 for j in range(per) if o * per + j >= GROUPZ - EDGE)

    def send_inner(o):
        e = edge_count(o)
        upper = low if o >= n // 2 else jnp.logical_not(low)
        send_part(mirrored(o), jnp.where(upper, 0, e), per - e)

    def send_bound(o):
        e = edge_count(o)
        upper = low if o >= n // 2 else jnp.logical_not(low)
        send_part(mirrored(o), jnp.where(upper, per - e, 0), e)

    def edge_copy(side):
        return pltpu.make_async_remote_copy(
            src_ref=edge_send.at[side], dst_ref=edge_recv.at[side],
            send_sem=es_sem.at[side], recv_sem=er_sem.at[side],
            device_id=(g + 1 - 2 * side, r), device_id_type=MESH,
        )

    def sends_to(side):
        return jnp.where(side == 0, g < groups - 1, g > 0)

    def gets_from(side):
        return jnp.where(side == 0, g > 0, g < groups - 1)

    def blend_edge(side):
        def store(j, value):
            edge_send[side, j] = value

        planes(store, base + jnp.where(side == 0, GROUPZ, -EDGE), EDGE)

    def send_edge(side):
        @pl.when(sends_to(side))
        def _():
            edge_copy(side).start()

    def add_edge(side):
        @pl.when(gets_from(side))
        def _():
            for p in range(EDGE):
                q = p + jnp.where(side == 0, 0, GROUPZ - EDGE)
                owner, j = q // per, q % per
                blend[owner, j] = (
                    blend[owner, j].astype(jnp.float32)
                    + edge_recv[side, p].astype(jnp.float32)
                ).astype(jnp.bfloat16)

    def wait_edge(side):
        @pl.when(gets_from(side))
        def _():
            edge_copy(side).wait_recv()

    edge_planes = list(range(EDGE)) + list(range(GROUPZ - EDGE, GROUPZ))
    bound = sorted({q // per for q in edge_planes}, reverse=True)
    free = [o for o in range(last, -1, -1) if o not in bound]
    far_side = jnp.where(low, 1, 0)

    load.wait()
    pl.semaphore_wait(barrier, n - 1 + jnp.where(has_below, 1, 0) + jnp.where(has_above, 1, 0))
    near_side = 1 - far_side
    far_free = [o for o in free if o >= n // 2]
    far_bound = [o for o in bound if o >= n // 2]
    near_free = [o for o in free if o < n // 2]
    near_bound = [o for o in bound if o < n // 2]

    for o in far_free:
        blend_owner(mirrored(o))
        send_owner(mirrored(o))
    blend_edge(far_side)
    send_edge(far_side)
    for o in far_bound:
        blend_owner(mirrored(o))
        send_inner(o)
    for o in near_free:
        blend_owner(mirrored(o))
        send_owner(mirrored(o))
    for o in near_bound:
        blend_owner(mirrored(o))
        send_inner(o)
    blend_edge(near_side)

    rec[...] = jnp.zeros_like(rec)
    for k in range(n):
        s = frame_start(k)
        totals = [0.0] * per
        for delta in (-1, 0, 1):
            group = jnp.clip(g + delta, 0, groups - 1)
            exists = jnp.where(group == g + delta, 1.0, 0.0)
            z0 = offs[0, group * n + k]
            wy = table[pl.ds(table_row(PADY + s - offs[1, group * n + k]), frame), :]
            for j in range(per):
                z = g * GROUPZ + r * per + j - z0
                totals[j] = totals[j] + wy * (rampz_at(z) * exists)
        for j in range(per):
            rec[j, s : s + frame] = rec[j, s : s + frame] + totals[j]
    rec[...] = 1.0 / jnp.maximum(rec[...], weight_floor)

    wait_edge(far_side)
    send_edge(near_side)
    add_edge(far_side)
    for o in far_bound:
        send_bound(o)
    acc[...] = jnp.zeros_like(acc)
    wait_edge(near_side)
    add_edge(near_side)
    for o in near_bound:
        send_bound(o)

    def add(k, source):
        s = pl.multiple_of(frame_start(k), 8)
        for j in range(per):
            acc[j, pl.ds(s, frame)] = acc[j, pl.ds(s, frame)] + source[j].astype(jnp.float32)

    add(r, blend.at[r])
    for i in range(1, n):
        k = ((r // 2 + i // 2) % (n // 2)) * 2 + (r + i) % 2
        pltpu.make_async_remote_copy(
            src_ref=blend.at[r], dst_ref=recv.at[k],
            send_sem=s_sem.at[k], recv_sem=r_sem.at[k],
            device_id=(g, k), device_id_type=MESH,
        ).wait_recv()
        add(k, recv.at[k])
    rows = out_ref.shape[1]
    for j in range(per):
        out_ref[j] = (acc[j, :rows] * rec[j, :rows]).astype(jnp.bfloat16)

    for i in range(1, n):
        k = lax.rem(r + i, n)
        pltpu.make_async_remote_copy(
            src_ref=blend.at[k], dst_ref=recv.at[r],
            send_sem=s_sem.at[k], recv_sem=r_sem.at[r],
            device_id=(g, k), device_id_type=MESH,
        ).wait_send()
    for side in range(2):
        @pl.when(sends_to(side))
        def _():
            edge_copy(side).wait_send()


def solution(mesh):
    groups, n = mesh.shape["slab"], mesh.shape["tile"]

    def shards(tiles, offsets, fracs):
        _, depth, tile_rows, cols = tiles.shape
        per = GROUPZ // n
        rows = (n - 1) * STEPY + tile_rows
        reach = max(
            min(k * STEPY + JITY, rows - tile_rows) + tile_rows - frame_start(k) for k in range(n)
        )
        frame = round_up(reach, 16)
        acc_rows = round_up(max(rows, frame_start(n - 1) + frame), 16)
        plane = ramp(tile_rows, RY)[:, None] * ramp(cols, RX)[None, :]
        table = np.zeros((round_up(PADY + frame + 8, 8), cols), np.float32)
        table[PADY : PADY + tile_rows] = plane
        rampz = np.zeros((depth + 2 * PADZ,), np.float32)
        rampz[PADZ : PADZ + depth] = ramp(depth, 2 * MARGIN)
        bf16, f32 = jnp.bfloat16, jnp.float32
        dma = pltpu.SemaphoreType.DMA
        return pl.pallas_call(
            functools.partial(kernel, groups, n, per, depth, tile_rows, frame, acc_rows),
            out_shape=pltpu.VMEM((per, rows, cols), bf16),
            in_specs=[pl.BlockSpec(memory_space=pltpu.SMEM)] * 3
            + [pl.BlockSpec(memory_space=pltpu.VMEM), pl.BlockSpec(memory_space=pl.ANY)],
            out_specs=pl.BlockSpec(memory_space=pltpu.VMEM),
            scratch_shapes=[
                pltpu.VMEM((depth + 1, tile_rows, cols), bf16),
                pltpu.VMEM((frame, 2 * tile_rows), bf16),
                pltpu.VMEM((frame, cols), f32),
                pltpu.VMEM((frame, cols), f32),
                pltpu.VMEM((n, per, frame, cols), bf16),
                pltpu.VMEM((2, EDGE, frame, cols), bf16),
                pltpu.VMEM((2, EDGE, frame, cols), bf16),
                pltpu.VMEM((n, per, frame, cols), bf16),
                pltpu.VMEM((per, acc_rows, cols), f32),
                pltpu.VMEM((per, acc_rows, cols), f32),
                dma, dma((2,)), dma((2,)), dma((n,)), dma((n,)),
            ],
            compiler_params=pltpu.CompilerParams(collective_id=0, has_side_effects=True),
        )(offsets.T, fracs.T, jnp.asarray(rampz), jnp.asarray(table), tiles)

    in_specs = (P(("slab", "tile"), None, None, None), P(), P())
    out_specs = P(("slab", "tile"), None, None)
    return jax.shard_map(shards, mesh=mesh, in_specs=in_specs, out_specs=out_specs, check_vma=False)
```

```python
import functools

import jax
import jax.numpy as jnp
import numpy as np
from jax import lax
from jax.experimental import pallas as pl
from jax.experimental.pallas import tpu as pltpu
from jax.sharding import PartitionSpec as P

GROUPZ = 16
MARGIN = 2
JIT = 1
STEPY = 230
JITY = 4
RY = 26
RX = 16
QUANT = 16
EDGE = MARGIN + JIT
PADY = 16
PADZ = 24

weight_floor = 0.05
MESH = pl.DeviceIdType.MESH


def ramp(length, ramp_width):
    position = np.arange(length, dtype=np.float64)
    rising = 0.5 - 0.5 * np.cos(np.pi * (position + 1.0) / (ramp_width + 1.0))
    rising = np.where(position < ramp_width, rising, 1.0)
    return np.minimum(rising, rising[::-1])


def frame_start(rank):
    if isinstance(rank, int):
        return max(rank * STEPY - JITY, 0)
    return jnp.maximum(rank * STEPY - JITY, 0)


def round_up(value, step):
    return -(-value // step) * step


def kernel(
    groups, n, per, depth, tile_rows, frame, acc_rows,
    offs_ref, fracs_ref, rampz_ref, table_ref, tile_ref, out_ref,
    raw, coef, wa, wb, blend, edge_send, edge_recv, recv, acc, rec,
    offs, fracs, rampz, table, small_sem, load_sem, es_sem, er_sem, s_sem, r_sem,
):
    g = lax.axis_index("slab")
    r = lax.axis_index("tile")
    me = g * n + r
    low = r < n // 2
    cols = raw.shape[2]
    last = n - 1

    barrier = pltpu.get_barrier_semaphore()
    for i in range(1, n):
        pl.semaphore_signal(
            barrier, inc=1, device_id=(g, lax.rem(r + i, n)), device_id_type=MESH
        )
    has_below = g > 0
    has_above = g < groups - 1

    @pl.when(has_below)
    def _():
        pl.semaphore_signal(barrier, inc=1, device_id=(g - 1, r), device_id_type=MESH)

    @pl.when(has_above)
    def _():
        pl.semaphore_signal(barrier, inc=1, device_id=(g + 1, r), device_id_type=MESH)

    smalls = [
        pltpu.make_async_copy(source, target, small_sem.at[i])
        for i, (source, target) in enumerate(
            [(offs_ref, offs), (fracs_ref, fracs), (rampz_ref, rampz), (table_ref, table)]
        )
    ]
    for small in smalls:
        small.start()
    load = pltpu.make_async_copy(tile_ref.at[0], raw.at[pl.ds(0, depth)], load_sem)
    load.start()

    def table_row(at):
        return jnp.clip(at, 0, table.shape[0] - frame)

    def rampz_at(z):
        return rampz[jnp.clip(z + PADZ, 0, rampz.shape[0] - 1)]

    for small in smalls:
        small.wait()
    corner = offs[0, me]
    shift = offs[1, me] - frame_start(r)
    fz = fracs[0, me].astype(jnp.float32) / QUANT
    fy = fracs[1, me].astype(jnp.float32) / QUANT
    fx = fracs[2, me].astype(jnp.float32) / QUANT
    row = lax.broadcasted_iota(jnp.int32, (frame, tile_rows), 0)
    col = lax.broadcasted_iota(jnp.int32, (frame, tile_rows), 1)
    behind = col - row + shift
    lerp_y = jnp.where(behind == 0, 1.0 - fy, jnp.where(behind == 1, fy, 0.0))
    coef[:, :tile_rows] = ((1.0 - fz) * lerp_y).astype(jnp.bfloat16)
    coef[:, tile_rows:] = (fz * lerp_y).astype(jnp.bfloat16)
    weight = table[pl.ds(table_row(PADY - shift), frame), :]
    lane = lax.broadcasted_iota(jnp.int32, (frame, cols), 1)
    wa[...] = weight * (1.0 - fx)
    wb[...] = jnp.where(lane < cols - 1, weight * fx, 0.0)
    raw[depth] = jnp.zeros(raw.shape[1:], raw.dtype)

    def planes(store, first, count):
        at = [jnp.clip(first + j, 0, depth - 1) for j in range(count)]
        top = jnp.concatenate([raw[z] for z in at], axis=1)
        bottom = jnp.concatenate([raw[z + 1] for z in at], axis=1)
        mixed = jnp.dot(
            coef[...], jnp.concatenate([top, bottom], axis=0),
            preferred_element_type=jnp.float32,
        )
        for j in range(count):
            part = mixed[:, j * cols : (j + 1) * cols]
            value = part * wa[...] + pltpu.roll(part, cols - 1, 1) * wb[...]
            store(j, (value * rampz_at(first + j)).astype(jnp.bfloat16))

    base = g * GROUPZ - corner

    def mirrored(owner):
        return jnp.where(low, owner, last - owner)

    def blend_owner(owner):
        def store(j, value):
            blend[owner, j] = value

        planes(store, base + owner * per, per)

    def send_owner(owner):
        @pl.when(owner != r)
        def _():
            pltpu.make_async_remote_copy(
                src_ref=blend.at[owner], dst_ref=recv.at[r],
                send_sem=s_sem.at[owner], recv_sem=r_sem.at[r],
                device_id=(g, owner), device_id_type=MESH,
            ).start()

    def send_part(owner, first, count):
        if count:
            @pl.when(owner != r)
            def _():
                part = pl.ds(first, count)
                pltpu.make_async_remote_copy(
                    src_ref=blend.at[owner, part], dst_ref=recv.at[r, part],
                    send_sem=s_sem.at[owner], recv_sem=r_sem.at[r],
                    device_id=(g, owner), device_id_type=MESH,
                ).start()

    def edge_count(o):
        o = max(o, last - o)
        return sum(1 for j in range(per) if o * per + j >= GROUPZ - EDGE)

    def send_inner(o):
        e = edge_count(o)
        upper = low if o >= n // 2 else jnp.logical_not(low)
        send_part(mirrored(o), jnp.where(upper, 0, e), per - e)

    def send_bound(o):
        e = edge_count(o)
        upper = low if o >= n // 2 else jnp.logical_not(low)
        send_part(mirrored(o), jnp.where(upper, per - e, 0), e)

    def edge_copy(side):
        return pltpu.make_async_remote_copy(
            src_ref=edge_send.at[side], dst_ref=edge_recv.at[side],
            send_sem=es_sem.at[side], recv_sem=er_sem.at[side],
            device_id=(g + 1 - 2 * side, r), device_id_type=MESH,
        )

    def sends_to(side):
        return jnp.where(side == 0, g < groups - 1, g > 0)

    def gets_from(side):
        return jnp.where(side == 0, g > 0, g < groups - 1)

    def blend_edge(side):
        def store(j, value):
            edge_send[side, j] = value

        planes(store, base + jnp.where(side == 0, GROUPZ, -EDGE), EDGE)

    def send_edge(side):
        @pl.when(sends_to(side))
        def _():
            edge_copy(side).start()

    def add_edge(side):
        @pl.when(gets_from(side))
        def _():
            for p in range(EDGE):
                q = p + jnp.where(side == 0, 0, GROUPZ - EDGE)
                owner, j = q // per, q % per
                blend[owner, j] = (
                    blend[owner, j].astype(jnp.float32)
                    + edge_recv[side, p].astype(jnp.float32)
                ).astype(jnp.bfloat16)

    def wait_edge(side):
        @pl.when(gets_from(side))
        def _():
            edge_copy(side).wait_recv()

    edge_planes = list(range(EDGE)) + list(range(GROUPZ - EDGE, GROUPZ))
    bound = sorted({q // per for q in edge_planes}, reverse=True)
    free = [o for o in range(last, -1, -1) if o not in bound]
    far_side = jnp.where(low, 1, 0)

    load.wait()
    pl.semaphore_wait(barrier, n - 1 + jnp.where(has_below, 1, 0) + jnp.where(has_above, 1, 0))
    near_side = 1 - far_side
    far_free = [o for o in free if o >= n // 2]
    far_bound = [o for o in bound if o >= n // 2]
    near_free = [o for o in free if o < n // 2]
    near_bound = [o for o in bound if o < n // 2]

    for o in far_free:
        blend_owner(mirrored(o))
        send_owner(mirrored(o))
    blend_edge(far_side)
    send_edge(far_side)
    for o in far_bound:
        blend_owner(mirrored(o))
        send_inner(o)
    for o in near_free:
        blend_owner(mirrored(o))
        send_owner(mirrored(o))
    for o in near_bound:
        blend_owner(mirrored(o))
        send_inner(o)
    blend_edge(near_side)

    rec[...] = jnp.zeros_like(rec)
    for k in range(n):
        s = frame_start(k)
        totals = [0.0] * per
        for delta in (-1, 0, 1):
            group = jnp.clip(g + delta, 0, groups - 1)
            exists = jnp.where(group == g + delta, 1.0, 0.0)
            z0 = offs[0, group * n + k]
            wy = table[pl.ds(table_row(PADY + s - offs[1, group * n + k]), frame), :]
            for j in range(per):
                z = g * GROUPZ + r * per + j - z0
                totals[j] = totals[j] + wy * (rampz_at(z) * exists)
        for j in range(per):
            rec[j, s : s + frame] = rec[j, s : s + frame] + totals[j]
    rec[...] = 1.0 / jnp.maximum(rec[...], weight_floor)

    wait_edge(far_side)
    send_edge(near_side)
    add_edge(far_side)
    for o in far_bound:
        send_bound(o)
    acc[...] = jnp.zeros_like(acc)
    wait_edge(near_side)
    add_edge(near_side)
    for o in near_bound:
        send_bound(o)

    def add(k, source):
        s = frame_start(k)
        for j in range(per):
            acc[j, pl.ds(s, frame)] = acc[j, pl.ds(s, frame)] + source[j].astype(jnp.float32)

    add(r, blend.at[r])
    for i in range(1, n):
        k = ((r // 2 + i // 2) % (n // 2)) * 2 + (r + i) % 2
        pltpu.make_async_remote_copy(
            src_ref=blend.at[r], dst_ref=recv.at[k],
            send_sem=s_sem.at[k], recv_sem=r_sem.at[k],
            device_id=(g, k), device_id_type=MESH,
        ).wait_recv()
        add(k, recv.at[k])
    rows = out_ref.shape[1]
    for j in range(per):
        out_ref[j] = (acc[j, :rows] * rec[j, :rows]).astype(jnp.bfloat16)

    for i in range(1, n):
        k = lax.rem(r + i, n)
        pltpu.make_async_remote_copy(
            src_ref=blend.at[k], dst_ref=recv.at[r],
            send_sem=s_sem.at[k], recv_sem=r_sem.at[r],
            device_id=(g, k), device_id_type=MESH,
        ).wait_send()
    for side in range(2):
        @pl.when(sends_to(side))
        def _():
            edge_copy(side).wait_send()


def solution(mesh):
    groups, n = mesh.shape["slab"], mesh.shape["tile"]

    def shards(tiles, offsets, fracs):
        _, depth, tile_rows, cols = tiles.shape
        per = GROUPZ // n
        rows = (n - 1) * STEPY + tile_rows
        reach = max(
            min(k * STEPY + JITY, rows - tile_rows) + tile_rows - frame_start(k) for k in range(n)
        )
        frame = round_up(reach, 8)
        acc_rows = round_up(max(rows, frame_start(n - 1) + frame), 16)
        plane = ramp(tile_rows, RY)[:, None] * ramp(cols, RX)[None, :]
        table = np.zeros((round_up(PADY + frame + 8, 8), cols), np.float32)
        table[PADY : PADY + tile_rows] = plane
        rampz = np.zeros((depth + 2 * PADZ,), np.float32)
        rampz[PADZ : PADZ + depth] = ramp(depth, 2 * MARGIN)
        bf16, f32 = jnp.bfloat16, jnp.float32
        dma = pltpu.SemaphoreType.DMA
        return pl.pallas_call(
            functools.partial(kernel, groups, n, per, depth, tile_rows, frame, acc_rows),
            out_shape=pltpu.VMEM((per, rows, cols), bf16),
            in_specs=[pl.BlockSpec(memory_space=pl.ANY)] * 5,
            out_specs=pl.BlockSpec(memory_space=pltpu.VMEM),
            scratch_shapes=[
                pltpu.VMEM((depth + 1, tile_rows, cols), bf16),
                pltpu.VMEM((frame, 2 * tile_rows), bf16),
                pltpu.VMEM((frame, cols), f32),
                pltpu.VMEM((frame, cols), f32),
                pltpu.VMEM((n, per, frame, cols), bf16),
                pltpu.VMEM((2, EDGE, frame, cols), bf16),
                pltpu.VMEM((2, EDGE, frame, cols), bf16),
                pltpu.VMEM((n, per, frame, cols), bf16),
                pltpu.VMEM((per, acc_rows, cols), f32),
                pltpu.VMEM((per, acc_rows, cols), f32),
                pltpu.SMEM((offsets.shape[1], offsets.shape[0]), jnp.int32),
                pltpu.SMEM((fracs.shape[1], fracs.shape[0]), jnp.int32),
                pltpu.SMEM(rampz.shape, f32),
                pltpu.VMEM(table.shape, f32),
                dma((4,)), dma, dma((2,)), dma((2,)), dma((n,)), dma((n,)),
            ],
            compiler_params=pltpu.CompilerParams(collective_id=0, has_side_effects=True),
        )(offsets.T, fracs.T, jnp.asarray(rampz), jnp.asarray(table), tiles)

    in_specs = (P(("slab", "tile"), None, None, None), P(), P())
    out_specs = P(("slab", "tile"), None, None)
    return jax.shard_map(shards, mesh=mesh, in_specs=in_specs, out_specs=out_specs, check_vma=False)
```

```python
import functools

import jax
import jax.numpy as jnp
import numpy as np
from jax import lax
from jax.experimental import pallas as pl
from jax.experimental.pallas import tpu as pltpu
from jax.sharding import PartitionSpec as P

GROUPZ = 16
MARGIN = 2
JIT = 1
STEPY = 230
JITY = 4
RY = 26
RX = 16
QUANT = 16
EDGE = MARGIN + JIT
PADY = 16
PADZ = 24

weight_floor = 0.05
MESH = pl.DeviceIdType.MESH


def ramp(length, ramp_width):
    position = np.arange(length, dtype=np.float64)
    rising = 0.5 - 0.5 * np.cos(np.pi * (position + 1.0) / (ramp_width + 1.0))
    rising = np.where(position < ramp_width, rising, 1.0)
    return np.minimum(rising, rising[::-1])


def frame_start(rank):
    if isinstance(rank, int):
        return max(rank * STEPY - JITY, 0)
    return jnp.maximum(rank * STEPY - JITY, 0)


def round_up(value, step):
    return -(-value // step) * step


def kernel(
    groups, n, per, depth, tile_rows, frame, acc_rows,
    offs_ref, fracs_ref, rampz_ref, table_ref, tile_ref, out_ref,
    raw, coef, wa, wb, blend, edge_send, edge_recv, recv, acc, rec,
    offs, fracs, rampz, table, small_sem, load_sem, es_sem, er_sem, s_sem, r_sem,
):
    g = lax.axis_index("slab")
    r = lax.axis_index("tile")
    me = g * n + r
    low = r < n // 2
    cols = raw.shape[2]
    last = n - 1

    barrier = pltpu.get_barrier_semaphore()
    for i in range(1, n):
        pl.semaphore_signal(
            barrier, inc=1, device_id=(g, lax.rem(r + i, n)), device_id_type=MESH
        )
    has_below = g > 0
    has_above = g < groups - 1

    @pl.when(has_below)
    def _():
        pl.semaphore_signal(barrier, inc=1, device_id=(g - 1, r), device_id_type=MESH)

    @pl.when(has_above)
    def _():
        pl.semaphore_signal(barrier, inc=1, device_id=(g + 1, r), device_id_type=MESH)

    smalls = [
        pltpu.make_async_copy(source, target, small_sem.at[i])
        for i, (source, target) in enumerate(
            [(offs_ref, offs), (fracs_ref, fracs), (rampz_ref, rampz), (table_ref, table)]
        )
    ]
    for small in smalls:
        small.start()
    load = pltpu.make_async_copy(tile_ref.at[0], raw.at[pl.ds(0, depth)], load_sem)
    load.start()

    def table_row(at):
        return jnp.clip(at, 0, table.shape[0] - frame)

    def rampz_at(z):
        return rampz[jnp.clip(z + PADZ, 0, rampz.shape[0] - 1)]

    for small in smalls:
        small.wait()
    corner = offs[0, me]
    shift = offs[1, me] - frame_start(r)
    fz = fracs[0, me].astype(jnp.float32) / QUANT
    fy = fracs[1, me].astype(jnp.float32) / QUANT
    fx = fracs[2, me].astype(jnp.float32) / QUANT
    row = lax.broadcasted_iota(jnp.int32, (frame, tile_rows), 0)
    col = lax.broadcasted_iota(jnp.int32, (frame, tile_rows), 1)
    behind = col - row + shift
    lerp_y = jnp.where(behind == 0, 1.0 - fy, jnp.where(behind == 1, fy, 0.0))
    coef[:, :tile_rows] = ((1.0 - fz) * lerp_y).astype(jnp.bfloat16)
    coef[:, tile_rows:] = (fz * lerp_y).astype(jnp.bfloat16)
    weight = table[pl.ds(table_row(PADY - shift), frame), :]
    lane = lax.broadcasted_iota(jnp.int32, (frame, cols), 1)
    wa[...] = weight * (1.0 - fx)
    wb[...] = jnp.where(lane < cols - 1, weight * fx, 0.0)
    raw[depth] = jnp.zeros(raw.shape[1:], raw.dtype)

    def planes(store, first, count):
        at = [jnp.clip(first + j, 0, depth - 1) for j in range(count)]
        top = jnp.concatenate([raw[z] for z in at], axis=1)
        bottom = jnp.concatenate([raw[z + 1] for z in at], axis=1)
        mixed = jnp.dot(
            coef[...], jnp.concatenate([top, bottom], axis=0),
            preferred_element_type=jnp.float32,
        )
        for j in range(count):
            part = mixed[:, j * cols : (j + 1) * cols]
            value = part * wa[...] + pltpu.roll(part, cols - 1, 1) * wb[...]
            store(j, (value * rampz_at(first + j)).astype(jnp.bfloat16))

    base = g * GROUPZ - corner

    def mirrored(owner):
        return jnp.where(low, owner, last - owner)

    def blend_owner(owner):
        def store(j, value):
            blend[owner, j] = value

        planes(store, base + owner * per, per)

    def send_owner(owner):
        @pl.when(owner != r)
        def _():
            pltpu.make_async_remote_copy(
                src_ref=blend.at[owner], dst_ref=recv.at[r],
                send_sem=s_sem.at[owner], recv_sem=r_sem.at[r],
                device_id=(g, owner), device_id_type=MESH,
            ).start()

    def send_part(owner, first, count):
        if count:
            @pl.when(owner != r)
            def _():
                part = pl.ds(first, count)
                pltpu.make_async_remote_copy(
                    src_ref=blend.at[owner, part], dst_ref=recv.at[r, part],
                    send_sem=s_sem.at[owner], recv_sem=r_sem.at[r],
                    device_id=(g, owner), device_id_type=MESH,
                ).start()

    def edge_count(o):
        o = max(o, last - o)
        return sum(1 for j in range(per) if o * per + j >= GROUPZ - EDGE)

    def send_inner(o):
        e = edge_count(o)
        upper = low if o >= n // 2 else jnp.logical_not(low)
        send_part(mirrored(o), jnp.where(upper, 0, e), per - e)

    def send_bound(o):
        e = edge_count(o)
        upper = low if o >= n // 2 else jnp.logical_not(low)
        send_part(mirrored(o), jnp.where(upper, per - e, 0), e)

    def edge_copy(side):
        return pltpu.make_async_remote_copy(
            src_ref=edge_send.at[side], dst_ref=edge_recv.at[side],
            send_sem=es_sem.at[side], recv_sem=er_sem.at[side],
            device_id=(g + 1 - 2 * side, r), device_id_type=MESH,
        )

    def sends_to(side):
        return jnp.where(side == 0, g < groups - 1, g > 0)

    def gets_from(side):
        return jnp.where(side == 0, g > 0, g < groups - 1)

    def blend_edge(side):
        def store(j, value):
            edge_send[side, j] = value

        planes(store, base + jnp.where(side == 0, GROUPZ, -EDGE), EDGE)

    def send_edge(side):
        @pl.when(sends_to(side))
        def _():
            edge_copy(side).start()

    def add_edge(side):
        @pl.when(gets_from(side))
        def _():
            for p in range(EDGE):
                q = p + jnp.where(side == 0, 0, GROUPZ - EDGE)
                owner, j = q // per, q % per
                blend[owner, j] = (
                    blend[owner, j].astype(jnp.float32)
                    + edge_recv[side, p].astype(jnp.float32)
                ).astype(jnp.bfloat16)

    def wait_edge(side):
        @pl.when(gets_from(side))
        def _():
            edge_copy(side).wait_recv()

    edge_planes = list(range(EDGE)) + list(range(GROUPZ - EDGE, GROUPZ))
    bound = sorted({q // per for q in edge_planes}, reverse=True)
    free = [o for o in range(last, -1, -1) if o not in bound]
    far_side = jnp.where(low, 1, 0)

    load.wait()
    pl.semaphore_wait(barrier, n - 1 + jnp.where(has_below, 1, 0) + jnp.where(has_above, 1, 0))
    near_side = 1 - far_side
    far_free = [o for o in free if o >= n // 2]
    far_bound = [o for o in bound if o >= n // 2]
    near_free = [o for o in free if o < n // 2]
    near_bound = [o for o in bound if o < n // 2]

    for o in far_free:
        blend_owner(mirrored(o))
        send_owner(mirrored(o))
    blend_edge(far_side)
    send_edge(far_side)
    for o in far_bound:
        blend_owner(mirrored(o))
        send_inner(o)
    for o in near_free:
        blend_owner(mirrored(o))
        send_owner(mirrored(o))
    for o in near_bound:
        blend_owner(mirrored(o))
        send_inner(o)
    blend_edge(near_side)

    rec[...] = jnp.zeros_like(rec)
    for k in range(n):
        s = frame_start(k)
        totals = [0.0] * per
        for delta in (-1, 0, 1):
            group = jnp.clip(g + delta, 0, groups - 1)
            exists = jnp.where(group == g + delta, 1.0, 0.0)
            z0 = offs[0, group * n + k]
            wy = table[pl.ds(table_row(PADY + s - offs[1, group * n + k]), frame), :]
            for j in range(per):
                z = g * GROUPZ + r * per + j - z0
                totals[j] = totals[j] + wy * (rampz_at(z) * exists)
        for j in range(per):
            rec[j, s : s + frame] = rec[j, s : s + frame] + totals[j]
    rec[...] = 1.0 / jnp.maximum(rec[...], weight_floor)

    wait_edge(far_side)
    send_edge(near_side)
    add_edge(far_side)
    for o in far_bound:
        send_bound(o)
    acc[...] = jnp.zeros_like(acc)
    wait_edge(near_side)
    add_edge(near_side)
    for o in near_bound:
        send_bound(o)

    def add(k, source):
        s = frame_start(k)
        for j in range(per):
            acc[j, pl.ds(s, frame)] = acc[j, pl.ds(s, frame)] + source[j].astype(jnp.float32)

    add(r, blend.at[r])
    for i in range(1, n):
        k = ((r // 2 + i // 2) % (n // 2)) * 2 + (r + i) % 2
        pltpu.make_async_remote_copy(
            src_ref=blend.at[r], dst_ref=recv.at[k],
            send_sem=s_sem.at[k], recv_sem=r_sem.at[k],
            device_id=(g, k), device_id_type=MESH,
        ).wait_recv()
        add(k, recv.at[k])
    rows = out_ref.shape[0]
    joined = (acc[:, :rows] * rec[:, :rows]).astype(jnp.bfloat16)
    out_ref[...] = jnp.swapaxes(joined, 0, 1)

    for i in range(1, n):
        k = lax.rem(r + i, n)
        pltpu.make_async_remote_copy(
            src_ref=blend.at[k], dst_ref=recv.at[r],
            send_sem=s_sem.at[k], recv_sem=r_sem.at[r],
            device_id=(g, k), device_id_type=MESH,
        ).wait_send()
    for side in range(2):
        @pl.when(sends_to(side))
        def _():
            edge_copy(side).wait_send()


def solution(mesh):
    groups, n = mesh.shape["slab"], mesh.shape["tile"]

    def shards(tiles, offsets, fracs):
        _, depth, tile_rows, cols = tiles.shape
        per = GROUPZ // n
        rows = (n - 1) * STEPY + tile_rows
        reach = max(
            min(k * STEPY + JITY, rows - tile_rows) + tile_rows - frame_start(k) for k in range(n)
        )
        frame = round_up(reach, 8)
        acc_rows = round_up(max(rows, frame_start(n - 1) + frame), 16)
        plane = ramp(tile_rows, RY)[:, None] * ramp(cols, RX)[None, :]
        table = np.zeros((round_up(PADY + frame + 8, 8), cols), np.float32)
        table[PADY : PADY + tile_rows] = plane
        rampz = np.zeros((depth + 2 * PADZ,), np.float32)
        rampz[PADZ : PADZ + depth] = ramp(depth, 2 * MARGIN)
        bf16, f32 = jnp.bfloat16, jnp.float32
        dma = pltpu.SemaphoreType.DMA
        joined = pl.pallas_call(
            functools.partial(kernel, groups, n, per, depth, tile_rows, frame, acc_rows),
            out_shape=pltpu.VMEM((rows, per, cols), bf16),
            in_specs=[pl.BlockSpec(memory_space=pl.ANY)] * 5,
            out_specs=pl.BlockSpec(memory_space=pltpu.VMEM),
            scratch_shapes=[
                pltpu.VMEM((depth + 1, tile_rows, cols), bf16),
                pltpu.VMEM((frame, 2 * tile_rows), bf16),
                pltpu.VMEM((frame, cols), f32),
                pltpu.VMEM((frame, cols), f32),
                pltpu.VMEM((n, per, frame, cols), bf16),
                pltpu.VMEM((2, EDGE, frame, cols), bf16),
                pltpu.VMEM((2, EDGE, frame, cols), bf16),
                pltpu.VMEM((n, per, frame, cols), bf16),
                pltpu.VMEM((per, acc_rows, cols), f32),
                pltpu.VMEM((per, acc_rows, cols), f32),
                pltpu.SMEM((offsets.shape[1], offsets.shape[0]), jnp.int32),
                pltpu.SMEM((fracs.shape[1], fracs.shape[0]), jnp.int32),
                pltpu.SMEM(rampz.shape, f32),
                pltpu.VMEM(table.shape, f32),
                dma((4,)), dma, dma((2,)), dma((2,)), dma((n,)), dma((n,)),
            ],
            compiler_params=pltpu.CompilerParams(collective_id=0, has_side_effects=True),
        )(offsets.T, fracs.T, jnp.asarray(rampz), jnp.asarray(table), tiles)
        return jnp.transpose(joined, (1, 0, 2))

    in_specs = (P(("slab", "tile"), None, None, None), P(), P())
    out_specs = P(("slab", "tile"), None, None)
    return jax.shard_map(shards, mesh=mesh, in_specs=in_specs, out_specs=out_specs, check_vma=False)
```
